32 devices in a mesh: grp: 16 (over z, y, core), dom: 2 (over x).
Axes of the slice: x: 2, y: 2, z: 4, core: 2. Of those that a mesh axis runs over, the one named last changes fastest.
Arguments:
- grids: float32 [32, 8, 64, 256], P('grp', None, None, 'dom'), may hold values from -6 to 6
- table: int32 [32, 8], P('grp'), may hold values from 0 to 15, all different within a row
- coefs: int32 [32], P('grp'), may hold values from -10 to 10, as said below
Outputs:
- combined: float32 [32, 8, 64, 256], P('grp', None, None, 'dom')
The draws below stay inside these ranges and needn't reach their ends.
Inputs may be any that keep to these rules, and one draw needn't show every extreme that they name: The 8 entries of a row of table differ, and every subspace is named by some row. `coefs`: every coefficient is one of 1, -5, 10, -10, 5, -1.
All inputs are finite; a program needn't handle non-finite values.
Results may differ from the reference program's by a relative error of at most 0.00007.
Values sent between devices are 32-bit elements; how exact they have to be, the bound alone decides.
A program may use at most 64 MiB of HBM per device.

```python
import jax
import jax.numpy as jnp
from jax import lax

FIELDS = 64
SLOTS = 8
GRIDS = 32
SUBS = 16
POINTS = 256


def draw_coefs(key, part):
    picks = jax.random.randint(jax.random.fold_in(key, 17), (GRIDS,), 0, 6)
    values = jnp.array([1, -5, 10, -10, 5, -1], dtype=jnp.int32)
    return values[picks].astype(jnp.int32)


def shard_levels(key, extent, pieces, smallest, largest):
    def one(axis_at, parts):
        heights = jax.random.uniform(jax.random.fold_in(jax.random.fold_in(key, 6), axis_at), (parts,), jnp.float32, smallest / len(pieces), largest / len(pieces))
        return jnp.repeat(jnp.exp(heights), extent[axis_at] // parts).reshape((-1,) + (1,) * (len(extent) - axis_at - 1))

    factor_of = one(*pieces[0])
    for cut in pieces[1:]:
        factor_of = factor_of * one(*cut)
    return factor_of


def choose_distinct(rng, rows, number_of, top, lift):
    order = jax.random.permutation(jax.random.fold_in(rng, 1), number_of)
    boost = order
    for power in range(3):
        boost = boost * boost // number_of
    boost = boost * lift // number_of
    tickets = jax.random.randint(jax.random.fold_in(rng, 2), (rows, number_of), 0, 4096) + boost
    fixed_rows = jax.random.permutation(jax.random.fold_in(rng, 3), rows)[jnp.arange(number_of) % rows]
    tickets = jnp.where(jnp.arange(rows)[:, None] == fixed_rows[None, :], 1 << 14, tickets)
    score = tickets * number_of + jnp.arange(number_of)
    return lax.top_k(score.astype(jnp.int32), top)[1].astype(jnp.int32)


def scatter_about(own_key, extent, width, bound, cuts=(), kind=jnp.bfloat16):
    factor_of = shard_levels(own_key, extent, cuts, -0.22, 0.18) if cuts else 1.0
    result = jax.random.normal(own_key, extent, jnp.float32) * width * factor_of
    return jnp.minimum(jnp.maximum(result, -bound), bound).astype(kind)


def setup_inputs(seed: int = 0) -> dict:
    splits = jax.random.split(jax.random.key(seed), 4)
    grids = scatter_about(splits[0], (GRIDS, SLOTS, FIELDS, POINTS), 1.0, 6.0, ((0, 16), (3, 2)), jnp.float32)
    table = choose_distinct(splits[1], GRIDS, SUBS, SLOTS, 0)
    coefs = draw_coefs(jax.random.fold_in(splits[3], 71), 0)
    return dict(grids=grids, table=table, coefs=coefs)


def reference(grids, table, coefs):
    count = GRIDS * SLOTS
    data = grids.reshape(count, FIELDS * POINTS)
    weight = jnp.repeat(coefs.astype(jnp.float32), SLOTS)
    labels = table.reshape(count).astype(jnp.int32)
    sparse = jax.ops.segment_sum(data * weight[:, None], labels, num_segments=SUBS)
    combined = sparse[labels]
    return combined.reshape(GRIDS, SLOTS, FIELDS, POINTS)
```

```python
import functools

import jax
import jax.numpy as jnp
from jax import lax
from jax.experimental import pallas as pl
from jax.experimental.pallas import tpu as pltpu
from jax.sharding import PartitionSpec as P

MESH = pl.DeviceIdType.MESH


def factors(n):
    rest = n // 2
    inner = 1 << ((rest.bit_length() - 1) // 2)
    assert n == 2 * inner * (rest // inner)
    return rest // inner, inner


def reduce_kernel(
    n, outer, inner, table, coefs, grids, full, local, part, from_core, from_inner, from_outer,
    load_sem, core_s, core_r, in_s, in_r, out_s, out_r, gout_s, gout_r, gin_s, gin_r, gcore_s, gcore_r,
):
    count, slots = grids.shape[:2]
    load = pltpu.make_async_copy(grids, local, load_sem)
    load.start()

    me = lax.axis_index("grp")
    core = lax.rem(me, 2)
    a = lax.rem(lax.div(me, 2), inner)
    b = lax.div(me, 2 * inner)

    def ident(ob, oa, oc):
        return (lax.rem(b + ob, outer) * inner + lax.rem(a + oa, inner)) * 2 + lax.rem(core + oc, 2)

    def remote(src, dst, send, recv, ob, oa, oc):
        return pltpu.make_async_remote_copy(
            src_ref=src, dst_ref=dst, send_sem=send, recv_sem=recv,
            device_id={"grp": ident(ob, oa, oc)}, device_id_type=MESH,
        )

    barrier = pltpu.get_barrier_semaphore()
    peers = [(0, 0, 1)] + [(0, oa, 0) for oa in range(1, inner)] + [(ob, 0, 0) for ob in range(1, outer)]
    for peer in peers:
        pl.semaphore_signal(barrier, inc=1, device_id={"grp": ident(*peer)}, device_id_type=MESH)

    order_b = sorted(range(1, outer), key=lambda o: -min(o, outer - o)) + [0]
    order_a = list(range(1, inner)) + [0]
    pieces = [(ob, oa) for ob in order_b for oa in order_a]

    weights = [coefs[g].astype(jnp.float32) for g in range(count)]
    labels = [[table[g, k] for k in range(slots)] for g in range(count)]

    def local_sum(sub):
        total = None
        for g in range(count):
            slot = jnp.int32(0)
            weight = jnp.float32(0)
            for k in range(slots):
                here = labels[g][k] == sub
                slot = jnp.where(here, jnp.int32(k), slot)
                weight = jnp.where(here, weights[g], weight)
            term = local[g, slot] * weight
            total = term if total is None else total + term
        return total

    load.wait()
    started = []

    def start(copy):
        copy.start()
        started.append(copy)

    first = True
    for ob, oa in pieces:
        part[ob, oa, 1] = local_sum(ident(ob, oa, 1))
        if first:
            pl.semaphore_wait(barrier, len(peers))
            first = False
        start(remote(part.at[ob, oa, 1], from_core.at[ob, oa], core_s.at[ob, oa], core_r.at[ob, oa], 0, 0, 1))
    for ob, oa in pieces:
        part[ob, oa, 0] = local_sum(ident(ob, oa, 0))

    for ob, oa in pieces:
        remote(part.at[ob, oa, 1], from_core.at[ob, oa], core_s.at[ob, oa], core_r.at[ob, oa], 0, 0, 1).wait_recv()
        if oa:
            part[ob, oa, 0] = part[ob, oa, 0] + from_core[ob, oa]
            start(remote(part.at[ob, oa, 0], from_inner.at[ob, oa], in_s.at[ob, oa], in_r.at[ob, oa], 0, oa, 0))
    for ob in order_b:
        total = part[ob, 0, 0] + from_core[ob, 0]
        for oa in range(1, inner):
            remote(part.at[ob, oa, 0], from_inner.at[ob, oa], in_s.at[ob, oa], in_r.at[ob, oa], 0, oa, 0).wait_recv()
            total = total + from_inner[ob, oa]
        if ob:
            part[ob, 0, 0] = total
            start(remote(part.at[ob, 0, 0], from_outer.at[ob], out_s.at[ob], out_r.at[ob], ob, 0, 0))
    for ob in order_b[:-1]:
        remote(part.at[ob, 0, 0], from_outer.at[ob], out_s.at[ob], out_r.at[ob], ob, 0, 0).wait_recv()
        total = total + from_outer[ob]
    full[me] = total

    def to_outer(o, chunk):
        return remote(full.at[chunk], full.at[chunk], gout_s.at[o], gout_r.at[o], o, 0, 0)

    def to_inner(ob, oa, chunk):
        return remote(full.at[chunk], full.at[chunk], gin_s.at[ob, oa], gin_r.at[ob, oa], 0, oa, 0)

    def to_core(ob, oa, chunk):
        return remote(full.at[chunk], full.at[chunk], gcore_s.at[ob, oa], gcore_r.at[ob, oa], 0, 0, 1)

    def spread(ob):
        chunk = ident(ob, 0, 0)
        for oa in range(1, inner):
            start(to_inner(ob, oa, chunk))
        start(to_core(ob, 0, chunk))

    for o in order_b[:-1]:
        start(to_outer(o, me))
    spread(0)
    near_first = order_b[:-1][::-1]
    for o in near_first:
        to_outer(o, ident(outer - o, 0, 0)).wait_recv()
        spread(outer - o)
    for ob in [0] + [outer - o for o in near_first]:
        for oa in range(1, inner):
            chunk = ident(ob, inner - oa, 0)
            to_inner(ob, oa, chunk).wait_recv()
            start(to_core(ob, inner - oa, chunk))
    for ob, oa in pieces:
        to_core(ob, oa, ident(ob, oa, 1)).wait_recv()
    for copy in started:
        copy.wait_send()


def pick_kernel(table, full, out, sems):
    count, slots = out.shape[:2]
    copies = []
    for g in range(count):
        for k in range(slots):
            copy = pltpu.make_async_copy(full.at[table[g, k]], out.at[g, k], sems.at[g, k])
            copy.start()
            copies.append(copy)
    for copy in copies:
        copy.wait()


def on_device(grids, table, coefs):
    count, slots, fields, points = grids.shape
    n = lax.axis_size("grp")
    outer, inner = factors(n)
    block = (fields, points)
    dma = pltpu.SemaphoreType.DMA
    smem = pl.BlockSpec(memory_space=pltpu.SMEM)
    vmem = pl.BlockSpec(memory_space=pltpu.VMEM)
    hbm = pl.BlockSpec(memory_space=pl.ANY)
    full = pl.pallas_call(
        functools.partial(reduce_kernel, n, outer, inner),
        out_shape=pltpu.VMEM((n,) + block, jnp.float32),
        in_specs=[smem, smem, hbm],
        out_specs=vmem,
        scratch_shapes=[
            pltpu.VMEM((count, slots) + block, jnp.float32),
            pltpu.VMEM((outer, inner, 2) + block, jnp.float32),
            pltpu.VMEM((outer, inner) + block, jnp.float32),
            pltpu.VMEM((outer, inner) + block, jnp.float32),
            pltpu.VMEM((outer,) + block, jnp.float32),
            dma,
        ]
        + [dma((outer, inner))] * 4
        + [dma((outer,))] * 4
        + [dma((outer, inner))] * 4,
        compiler_params=pltpu.CompilerParams(collective_id=0, has_side_effects=True),
        name="reduce_all",
    )(table, coefs, grids)
    return pl.pallas_call(
        pick_kernel,
        out_shape=jax.ShapeDtypeStruct(grids.shape, jnp.float32),
        in_specs=[smem, vmem],
        out_specs=hbm,
        scratch_shapes=[dma((count, slots))],
        name="pick",
    )(table, pltpu.with_memory_space_constraint(full, pltpu.VMEM))


def solution(mesh):
    return jax.shard_map(
        on_device,
        mesh=mesh,
        in_specs=(P("grp", None, None, "dom"), P("grp", None), P("grp")),
        out_specs=P("grp", None, None, "dom"),
        check_vma=False,
    )
```

```python
import functools

import jax
import jax.numpy as jnp
from jax import lax
from jax.experimental import pallas as pl
from jax.experimental.pallas import tpu as pltpu
from jax.sharding import PartitionSpec as P

MESH = pl.DeviceIdType.MESH


def factors(n):
    rest = n // 2
    inner = 1 << ((rest.bit_length() - 1) // 2)
    assert n == 2 * inner * (rest // inner)
    return rest // inner, inner


def reduce_kernel(
    n, outer, inner, spread_by, table, coefs, grids, out, local, part, from_core, from_inner, from_outer, full,
    load_sem, core_s, core_r, in_s, in_r, gin_s, gin_r, gcore_s, gcore_r, out_s, out_r, gout_s, gout_r,
):
    count, slots = grids.shape[:2]
    load = pltpu.make_async_copy(grids, local, load_sem)
    load.start()

    me = lax.axis_index("grp")
    core = lax.rem(me, 2)
    a = lax.rem(lax.div(me, 2), inner)
    b = lax.div(me, 2 * inner)

    owners = outer // spread_by
    base = (outer - owners) // 2
    half = outer // 2
    upper = lax.div(b, max(half, 1)) if half else 0
    is_owner = (b >= base) & (b < base + owners)

    def chunk_at(j):
        return lax.rem((1 - upper) * half + j, outer)

    def position(i):
        return lax.rem(i - (1 - upper) * half + outer, outer)

    def owner(i):
        return base + lax.div(i, spread_by)

    def ident(i, oa, oc):
        return (i * inner + lax.rem(a + oa, inner)) * 2 + lax.rem(core + oc, 2)

    def remote(src, dst, send, recv, device):
        return pltpu.make_async_remote_copy(
            src_ref=src, dst_ref=dst, send_sem=send, recv_sem=recv,
            device_id={"grp": device}, device_id_type=MESH,
        )

    partner = ident(b, 0, 1)

    def outer_peer(d):
        return ident(lax.rem(b + d, outer), 0, 0)

    barrier = pltpu.get_barrier_semaphore()
    peers = [outer_peer(d) for d in range(1, outer)] + [ident(b, oa, 0) for oa in range(1, inner)] + [partner]
    for peer in peers:
        pl.semaphore_signal(barrier, inc=1, device_id={"grp": peer}, device_id_type=MESH)

    order_a = list(range(1, inner)) + [0]
    pieces = [(j, oa) for j in range(outer) for oa in order_a]

    weights = [coefs[g].astype(jnp.float32) for g in range(count)]
    labels = [[table[g, k] for k in range(slots)] for g in range(count)]

    def local_sum(sub):
        total = None
        for g in range(count):
            slot = jnp.int32(0)
            weight = jnp.float32(0)
            for k in range(slots):
                here = labels[g][k] == sub
                slot = jnp.where(here, jnp.int32(k), slot)
                weight = jnp.where(here, weights[g], weight)
            term = local[g, slot] * weight
            total = term if total is None else total + term
        return total

    started = []

    def start(copy, when=None):
        if when is None:
            copy.start()
        else:
            pl.when(when)(copy.start)
        started.append((copy, when))

    def core_copy(j, oa):
        return remote(part.at[j, oa, 1], from_core.at[j, oa], core_s.at[j, oa], core_r.at[j, oa], partner)

    def inner_copy(j, oa):
        return remote(part.at[j, oa, 0], from_inner.at[j, oa], in_s.at[j, oa], in_r.at[j, oa], ident(b, oa, 0))

    def outer_copy(j):
        i = chunk_at(j)
        to = owner(i)
        slot, behind = lax.rem(i, spread_by), lax.rem(b - to + outer, outer)
        return remote(
            part.at[j, 0, 0], from_outer.at[slot, behind], out_s.at[j], out_r.at[slot, behind], ident(to, 0, 0)
        ), to != b

    load.wait()
    for j, oa in pieces:
        part[j, oa, 1] = local_sum(ident(chunk_at(j), oa, 1))
    for j, oa in pieces:
        part[j, oa, 0] = local_sum(ident(chunk_at(j), oa, 0))
    pl.semaphore_wait(barrier, len(peers))
    for j, oa in pieces:
        start(core_copy(j, oa))

    for j, oa in pieces:
        core_copy(j, oa).wait_recv()
        if oa:
            part[j, oa, 0] = part[j, oa, 0] + from_core[j, oa]
            start(inner_copy(j, oa))
    for j in range(outer):
        total = part[j, 0, 0] + from_core[j, 0]
        for oa in range(1, inner):
            inner_copy(j, oa).wait_recv()
            total = total + from_inner[j, oa]
        part[j, 0, 0] = total
        start(*outer_copy(j))

    def from_owner(i, d, send):
        chunk = ident(i, 0, 0)
        return remote(full.at[chunk], full.at[chunk], send, gout_r.at[i], outer_peer(d))

    def to_inner(j, oa, source):
        chunk = ident(chunk_at(j), source, 0)
        return remote(full.at[chunk], full.at[chunk], gin_s.at[j, oa], gin_r.at[j, oa], ident(b, oa, 0))

    def to_core(j, source, oc):
        chunk = ident(chunk_at(j), source, oc)
        return remote(full.at[chunk], full.at[chunk], gcore_s.at[j, source], gcore_r.at[j, source], partner)

    far_first = sorted(range(1, outer), key=lambda d: -min(d, outer - d))
    along = 1 - 2 * upper

    def final(slot):
        i = (b - base) * spread_by + slot
        total = part[position(i), 0, 0]
        for d in range(1, outer):
            remote(
                part.at[0, 0, 0], from_outer.at[slot, d], out_s.at[0], out_r.at[slot, d], outer_peer(d)
            ).wait_recv()
            total = total + from_outer[slot, d]
        full[ident(i, 0, 0)] = total
        for d in far_first:
            from_owner(i, lax.rem(along * d + outer, outer), gout_s.at[slot, d]).start()

    @pl.when(is_owner)
    def _():
        for slot in range(spread_by):
            final(slot)

    near_first = list(range(half, outer)) + list(range(half))
    for j in near_first:
        i = chunk_at(j)

        @pl.when(owner(i) != b)
        def _():
            from_owner(i, 1, gout_s.at[0, 0]).wait_recv()

        for oa in range(1, inner):
            start(to_inner(j, oa, 0))
        start(to_core(j, 0, 0))
    for j in near_first:
        for oa in range(1, inner):
            to_inner(j, oa, inner - oa).wait_recv()
            start(to_core(j, inner - oa, 0))
    for j in near_first:
        for oa in range(inner):
            to_core(j, oa, 1).wait_recv()
    for g in range(count):
        for k in range(slots):
            out[g, k] = full[labels[g][k]]

    for copy, when in started:
        if when is None:
            copy.wait_send()
        else:
            pl.when(when)(copy.wait_send)

    @pl.when(is_owner)
    def _():
        for slot in range(spread_by):
            for d in far_first:
                i = (b - base) * spread_by + slot
                from_owner(i, lax.rem(along * d + outer, outer), gout_s.at[slot, d]).wait_send()


def on_device(grids, table, coefs):
    count, slots, fields, points = grids.shape
    n = lax.axis_size("grp")
    outer, inner = factors(n)
    spread_by = 2 if outer % 4 == 0 else 1
    block = (fields, points)
    dma = pltpu.SemaphoreType.DMA
    smem = pl.BlockSpec(memory_space=pltpu.SMEM)
    return pl.pallas_call(
        functools.partial(reduce_kernel, n, outer, inner, spread_by),
        out_shape=pltpu.VMEM(grids.shape, jnp.float32),
        in_specs=[smem, smem, pl.BlockSpec(memory_space=pl.ANY)],
        out_specs=pl.BlockSpec(memory_space=pltpu.VMEM),
        scratch_shapes=[
            pltpu.VMEM((count, slots) + block, jnp.float32),
            pltpu.VMEM((outer, inner, 2) + block, jnp.float32),
            pltpu.VMEM((outer, inner) + block, jnp.float32),
            pltpu.VMEM((outer, inner) + block, jnp.float32),
            pltpu.VMEM((spread_by, outer) + block, jnp.float32),
            pltpu.VMEM((n,) + block, jnp.float32),
            dma,
        ]
        + [dma((outer, inner))] * 8
        + [dma((outer,)), dma((spread_by, outer)), dma((spread_by, outer)), dma((outer,))],
        compiler_params=pltpu.CompilerParams(collective_id=0, has_side_effects=True),
        name="reduce_all",
    )(table, coefs, grids)


def solution(mesh):
    return jax.shard_map(
        on_device,
        mesh=mesh,
        in_specs=(P("grp", None, None, "dom"), P("grp", None), P("grp")),
        out_specs=P("grp", None, None, "dom"),
        check_vma=False,
    )
```

```python
import functools

import jax
import jax.numpy as jnp
from jax import lax
from jax.experimental import pallas as pl
from jax.experimental.pallas import tpu as pltpu
from jax.sharding import PartitionSpec as P

MESH = pl.DeviceIdType.MESH


def factors(n):
    rest = n // 2
    inner = 1 << ((rest.bit_length() - 1) // 2)
    assert n == 2 * inner * (rest // inner)
    return rest // inner, inner


def reduce_kernel(
    n, outer, inner, spread_by, table, coefs, grids, out, local, part, from_core, from_inner, from_outer, full,
    load_sem, core_s, core_r, in_s, in_r, gin_s, gin_r, gcore_s, gcore_r, out_s, out_r, gout_s, gout_r,
):
    count, slots = grids.shape[:2]
    load = pltpu.make_async_copy(grids, local, load_sem)
    load.start()

    me = lax.axis_index("grp")
    core = lax.rem(me, 2)
    a = lax.rem(lax.div(me, 2), inner)
    b = lax.div(me, 2 * inner)

    owners = outer // spread_by
    base = (outer - owners) // 2
    half = outer // 2
    upper = lax.div(b, max(half, 1)) if half else 0
    is_owner = (b >= base) & (b < base + owners)

    def chunk_at(j):
        return lax.rem((1 - upper) * half + j, outer)

    def position(i):
        return lax.rem(i - (1 - upper) * half + outer, outer)

    def owner(i):
        return base + lax.div(i, spread_by)

    def ident(i, oa, oc):
        return (i * inner + lax.rem(a + oa, inner)) * 2 + lax.rem(core + oc, 2)

    def remote(src, dst, send, recv, device):
        return pltpu.make_async_remote_copy(
            src_ref=src, dst_ref=dst, send_sem=send, recv_sem=recv,
            device_id={"grp": device}, device_id_type=MESH,
        )

    partner = ident(b, 0, 1)

    def outer_peer(d):
        return ident(lax.rem(b + d, outer), 0, 0)

    barrier = pltpu.get_barrier_semaphore()
    def signal(peer):
        pl.semaphore_signal(barrier, inc=1, device_id={"grp": peer}, device_id_type=MESH)

    for d in sorted(range(1, outer), key=lambda d: -min(d, outer - d)):
        to = lax.rem(b + d, outer)

        @pl.when(is_owner | ((to >= base) & (to < base + owners)))
        def _():
            signal(ident(to, 0, 0))

    for oa in range(1, inner):
        signal(ident(b, oa, 0))
    signal(partner)
    arrivals = inner + jnp.where(is_owner, outer - 1, owners)

    order_a = list(range(1, inner)) + [0]
    pieces = [(j, oa) for j in range(outer) for oa in order_a]

    weights = [coefs[g].astype(jnp.float32) for g in range(count)]
    labels = [[table[g, k] for k in range(slots)] for g in range(count)]

    def local_sum(sub):
        total = None
        for g in range(count):
            slot = jnp.int32(0)
            weight = jnp.float32(0)
            for k in range(slots):
                here = labels[g][k] == sub
                slot = jnp.where(here, jnp.int32(k), slot)
                weight = jnp.where(here, weights[g], weight)
            term = local[g, slot] * weight
            total = term if total is None else total + term
        return total

    started = []

    def start(copy, when=None):
        if when is None:
            copy.start()
        else:
            pl.when(when)(copy.start)
        started.append((copy, when))

    def core_copy(j, oa):
        return remote(part.at[j, oa, 1], from_core.at[j, oa], core_s.at[j, oa], core_r.at[j, oa], partner)

    def inner_copy(j, oa):
        return remote(part.at[j, oa, 0], from_inner.at[j, oa], in_s.at[j, oa], in_r.at[j, oa], ident(b, oa, 0))

    def outer_copy(j):
        i = chunk_at(j)
        to = owner(i)
        slot, behind = lax.rem(i, spread_by), lax.rem(b - to + outer, outer)
        return remote(
            part.at[j, 0, 0], from_outer.at[slot, behind], out_s.at[j], out_r.at[slot, behind], ident(to, 0, 0)
        ), to != b

    load.wait()
    for j, oa in pieces:
        part[j, oa, 1] = local_sum(ident(chunk_at(j), oa, 1))
    for j, oa in pieces:
        part[j, oa, 0] = local_sum(ident(chunk_at(j), oa, 0))
    pl.semaphore_wait(barrier, arrivals)
    for j, oa in pieces:
        start(core_copy(j, oa))

    for j, oa in pieces:
        core_copy(j, oa).wait_recv()
        if oa:
            part[j, oa, 0] = part[j, oa, 0] + from_core[j, oa]
            start(inner_copy(j, oa))
    for j in range(outer):
        total = part[j, 0, 0] + from_core[j, 0]
        for oa in range(1, inner):
            inner_copy(j, oa).wait_recv()
            total = total + from_inner[j, oa]
        part[j, 0, 0] = total
        start(*outer_copy(j))

    def from_owner(i, d, send):
        chunk = ident(i, 0, 0)
        return remote(full.at[chunk], full.at[chunk], send, gout_r.at[i], outer_peer(d))

    def to_inner(j, oa, source):
        chunk = ident(chunk_at(j), source, 0)
        return remote(full.at[chunk], full.at[chunk], gin_s.at[j, oa], gin_r.at[j, oa], ident(b, oa, 0))

    def to_core(j, source, oc):
        chunk = ident(chunk_at(j), source, oc)
        return remote(full.at[chunk], full.at[chunk], gcore_s.at[j, source], gcore_r.at[j, source], partner)

    far_first = sorted(range(1, outer), key=lambda d: -min(d, outer - d))
    along = 1 - 2 * upper

    def final(slot):
        i = (b - base) * spread_by + slot
        total = part[position(i), 0, 0]
        for d in range(1, outer):
            remote(
                part.at[0, 0, 0], from_outer.at[slot, d], out_s.at[0], out_r.at[slot, d], outer_peer(d)
            ).wait_recv()
            total = total + from_outer[slot, d]
        full[ident(i, 0, 0)] = total
        for d in far_first:
            from_owner(i, lax.rem(along * d + outer, outer), gout_s.at[slot, d]).start()

    @pl.when(is_owner)
    def _():
        for slot in range(spread_by):
            final(slot)

    near_first = list(range(half, outer)) + list(range(half))
    for j in near_first:
        i = chunk_at(j)

        @pl.when(owner(i) != b)
        def _():
            from_owner(i, 1, gout_s.at[0, 0]).wait_recv()

        for oa in range(1, inner):
            start(to_inner(j, oa, 0))
        start(to_core(j, 0, 0))
    for j in near_first:
        for oa in range(1, inner):
            to_inner(j, oa, inner - oa).wait_recv()
            start(to_core(j, inner - oa, 0))
    for j in near_first:
        for oa in range(inner):
            to_core(j, oa, 1).wait_recv()
    for g in range(count):
        for k in range(slots):
            out[g, k] = full[labels[g][k]]

    for copy, when in started:
        if when is None:
            copy.wait_send()
        else:
            pl.when(when)(copy.wait_send)

    @pl.when(is_owner)
    def _():
        for slot in range(spread_by):
            for d in far_first:
                i = (b - base) * spread_by + slot
                from_owner(i, lax.rem(along * d + outer, outer), gout_s.at[slot, d]).wait_send()


def on_device(grids, table, coefs):
    count, slots, fields, points = grids.shape
    n = lax.axis_size("grp")
    outer, inner = factors(n)
    spread_by = 2 if outer % 4 == 0 else 1
    block = (fields, points)
    dma = pltpu.SemaphoreType.DMA
    smem = pl.BlockSpec(memory_space=pltpu.SMEM)
    return pl.pallas_call(
        functools.partial(reduce_kernel, n, outer, inner, spread_by),
        out_shape=pltpu.VMEM(grids.shape, jnp.float32),
        in_specs=[smem, smem, pl.BlockSpec(memory_space=pl.ANY)],
        out_specs=pl.BlockSpec(memory_space=pltpu.VMEM),
        scratch_shapes=[
            pltpu.VMEM((count, slots) + block, jnp.float32),
            pltpu.VMEM((outer, inner, 2) + block, jnp.float32),
            pltpu.VMEM((outer, inner) + block, jnp.float32),
            pltpu.VMEM((outer, inner) + block, jnp.float32),
            pltpu.VMEM((spread_by, outer) + block, jnp.float32),
            pltpu.VMEM((n,) + block, jnp.float32),
            dma,
        ]
        + [dma((outer, inner))] * 8
        + [dma((outer,)), dma((spread_by, outer)), dma((spread_by, outer)), dma((outer,))],
        compiler_params=pltpu.CompilerParams(collective_id=0, has_side_effects=True),
        name="reduce_all",
    )(table, coefs, grids)


def solution(mesh):
    return jax.shard_map(
        on_device,
        mesh=mesh,
        in_specs=(P("grp", None, None, "dom"), P("grp", None), P("grp")),
        out_specs=P("grp", None, None, "dom"),
        check_vma=False,
    )
```

```python
import functools

import jax
import jax.numpy as jnp
from jax import lax
from jax.experimental import pallas as pl
from jax.experimental.pallas import tpu as pltpu
from jax.sharding import PartitionSpec as P

MESH = pl.DeviceIdType.MESH


def factors(n):
    rest = n // 2
    inner = 1 << ((rest.bit_length() - 1) // 2)
    assert n == 2 * inner * (rest // inner)
    return rest // inner, inner


def reduce_kernel(
    n, outer, inner, spread_by, table_in, coefs_in, grids, out, table, coefs, local, part, from_core, from_inner, from_outer, full,
    load_sem, table_sem, coefs_sem, core_s, core_r, in_s, in_r, gin_s, gin_r, gcore_s, gcore_r, out_s, out_r, gout_s, gout_r,
):
    count, slots = grids.shape[:2]
    me = lax.axis_index("grp")
    core = lax.rem(me, 2)
    a = lax.rem(lax.div(me, 2), inner)
    b = lax.div(me, 2 * inner)

    owners = outer // spread_by
    base = (outer - owners) // 2
    half = outer // 2
    upper = lax.div(b, max(half, 1)) if half else 0
    is_owner = (b >= base) & (b < base + owners)

    def chunk_at(j):
        return lax.rem((1 - upper) * half + j, outer)

    def position(i):
        return lax.rem(i - (1 - upper) * half + outer, outer)

    def owner(i):
        return base + lax.div(i, spread_by)

    def ident(i, oa, oc):
        return (i * inner + lax.rem(a + oa, inner)) * 2 + lax.rem(core + oc, 2)

    def remote(src, dst, send, recv, device):
        return pltpu.make_async_remote_copy(
            src_ref=src, dst_ref=dst, send_sem=send, recv_sem=recv,
            device_id={"grp": device}, device_id_type=MESH,
        )

    partner = ident(b, 0, 1)

    def outer_peer(d):
        return ident(lax.rem(b + d, outer), 0, 0)

    barrier = pltpu.get_barrier_semaphore()
    def signal(peer):
        pl.semaphore_signal(barrier, inc=1, device_id={"grp": peer}, device_id_type=MESH)

    for d in sorted(range(1, outer), key=lambda d: -min(d, outer - d)):
        to = lax.rem(b + d, outer)

        @pl.when(is_owner | ((to >= base) & (to < base + owners)))
        def _():
            signal(ident(to, 0, 0))

    for oa in range(1, inner):
        signal(ident(b, oa, 0))
    signal(partner)
    arrivals = inner + jnp.where(is_owner, outer - 1, owners)

    loads = [
        pltpu.make_async_copy(table_in, table, table_sem),
        pltpu.make_async_copy(coefs_in, coefs, coefs_sem),
        pltpu.make_async_copy(grids, local, load_sem),
    ]
    for load in loads:
        load.start()

    order_a = list(range(1, inner)) + [0]
    pieces = [(j, oa) for oa in order_a for j in range(outer)]

    for load in loads[:2]:
        load.wait()
    weights = [coefs[g].astype(jnp.float32) for g in range(count)]
    labels = [[table[g, k] for k in range(slots)] for g in range(count)]

    def local_sum(sub):
        total = None
        for g in range(count):
            slot = jnp.int32(0)
            weight = jnp.float32(0)
            for k in range(slots):
                here = labels[g][k] == sub
                slot = jnp.where(here, jnp.int32(k), slot)
                weight = jnp.where(here, weights[g], weight)
            term = local[g, slot] * weight
            total = term if total is None else total + term
        return total

    started = []

    def start(copy, when=None):
        if when is None:
            copy.start()
        else:
            pl.when(when)(copy.start)
        started.append((copy, when))

    def core_copy(j, oa):
        return remote(part.at[j, oa, 1], from_core.at[j, oa], core_s.at[j, oa], core_r.at[j, oa], partner)

    def inner_copy(j, oa):
        return remote(part.at[j, oa, 0], from_inner.at[j, oa], in_s.at[j, oa], in_r.at[j, oa], ident(b, oa, 0))

    def outer_copy(j):
        i = chunk_at(j)
        to = owner(i)
        slot, behind = lax.rem(i, spread_by), lax.rem(b - to + outer, outer)
        return remote(
            part.at[j, 0, 0], from_outer.at[slot, behind], out_s.at[j], out_r.at[slot, behind], ident(to, 0, 0)
        ), to != b

    loads[2].wait()
    for j, oa in pieces:
        part[j, oa, 1] = local_sum(ident(chunk_at(j), oa, 1))
    for j, oa in pieces:
        part[j, oa, 0] = local_sum(ident(chunk_at(j), oa, 0))
    pl.semaphore_wait(barrier, arrivals)
    for j, oa in pieces:
        start(core_copy(j, oa))

    for j, oa in pieces:
        core_copy(j, oa).wait_recv()
        if oa:
            part[j, oa, 0] = part[j, oa, 0] + from_core[j, oa]
            start(inner_copy(j, oa))
    for j in range(outer):
        total = part[j, 0, 0] + from_core[j, 0]
        for oa in range(1, inner):
            inner_copy(j, oa).wait_recv()
            total = total + from_inner[j, oa]
        part[j, 0, 0] = total
        start(*outer_copy(j))

    def from_owner(i, d, send):
        chunk = ident(i, 0, 0)
        return remote(full.at[chunk], full.at[chunk], send, gout_r.at[i], outer_peer(d))

    def to_inner(j, oa, source):
        chunk = ident(chunk_at(j), source, 0)
        return remote(full.at[chunk], full.at[chunk], gin_s.at[j, oa], gin_r.at[j, oa], ident(b, oa, 0))

    def to_core(j, source, oc):
        chunk = ident(chunk_at(j), source, oc)
        return remote(full.at[chunk], full.at[chunk], gcore_s.at[j, source], gcore_r.at[j, source], partner)

    far_first = sorted(range(1, outer), key=lambda d: -min(d, outer - d))
    along = 1 - 2 * upper

    def final(slot):
        i = (b - base) * spread_by + slot
        total = part[position(i), 0, 0]
        for d in range(1, outer):
            remote(
                part.at[0, 0, 0], from_outer.at[slot, d], out_s.at[0], out_r.at[slot, d], outer_peer(d)
            ).wait_recv()
            total = total + from_outer[slot, d]
        full[ident(i, 0, 0)] = total
        for d in far_first:
            from_owner(i, lax.rem(along * d + outer, outer), gout_s.at[slot, d]).start()
        for oa in range(1, inner):
            to_inner(position(i), oa, 0).start()
        to_core(position(i), 0, 0).start()

    @pl.when(is_owner)
    def _():
        for slot in range(spread_by):
            final(slot)

    near_first = list(range(half, outer)) + list(range(half))
    for j in near_first:
        i = chunk_at(j)

        @pl.when(owner(i) != b)
        def _():
            from_owner(i, 1, gout_s.at[0, 0]).wait_recv()
            for oa in range(1, inner):
                to_inner(j, oa, 0).start()
            to_core(j, 0, 0).start()

        for oa in range(1, inner):
            started.append((to_inner(j, oa, 0), None))
        started.append((to_core(j, 0, 0), None))
    for j in near_first:
        for oa in range(1, inner):
            to_inner(j, oa, inner - oa).wait_recv()
            start(to_core(j, inner - oa, 0))
    for j in near_first:
        for oa in range(inner):
            to_core(j, oa, 1).wait_recv()
    for g in range(count):
        for k in range(slots):
            out[g, k] = full[labels[g][k]]

    for copy, when in started:
        if when is None:
            copy.wait_send()
        else:
            pl.when(when)(copy.wait_send)

    @pl.when(is_owner)
    def _():
        for slot in range(spread_by):
            for d in far_first:
                i = (b - base) * spread_by + slot
                from_owner(i, lax.rem(along * d + outer, outer), gout_s.at[slot, d]).wait_send()


def on_device(grids, table, coefs):
    count, slots, fields, points = grids.shape
    n = lax.axis_size("grp")
    outer, inner = factors(n)
    spread_by = 2 if outer % 4 == 0 else 1
    block = (fields, points)
    dma = pltpu.SemaphoreType.DMA
    return pl.pallas_call(
        functools.partial(reduce_kernel, n, outer, inner, spread_by),
        out_shape=pltpu.VMEM(grids.shape, jnp.float32),
        in_specs=[pl.BlockSpec(memory_space=pl.ANY)] * 3,
        out_specs=pl.BlockSpec(memory_space=pltpu.VMEM),
        scratch_shapes=[
            pltpu.SMEM(table.shape, jnp.int32),
            pltpu.SMEM(coefs.shape, jnp.int32),
            pltpu.VMEM((count, slots) + block, jnp.float32),
            pltpu.VMEM((outer, inner, 2) + block, jnp.float32),
            pltpu.VMEM((outer, inner) + block, jnp.float32),
            pltpu.VMEM((outer, inner) + block, jnp.float32),
            pltpu.VMEM((spread_by, outer) + block, jnp.float32),
            pltpu.VMEM((n,) + block, jnp.float32),
            dma,
            dma,
            dma,
        ]
        + [dma((outer, inner))] * 8
        + [dma((outer,)), dma((spread_by, outer)), dma((spread_by, outer)), dma((outer,))],
        compiler_params=pltpu.CompilerParams(collective_id=0, has_side_effects=True),
        name="reduce_all",
    )(table, coefs, grids)


def solution(mesh):
    return jax.shard_map(
        on_device,
        mesh=mesh,
        in_specs=(P("grp", None, None, "dom"), P("grp", None), P("grp")),
        out_specs=P("grp", None, None, "dom"),
        check_vma=False,
    )
```
